32 devices in a mesh: row: 2 (over x), col: 4 (over y, core), layer: 4 (over z).
Axes of the slice: x: 2, y: 2, z: 4, core: 2. Of those that a mesh axis runs over, the one named last changes fastest.
Arguments:
- a_cyclic: float32 [4, 1024, 4096], P('layer', 'row', 'col'), may hold values from -6 to 6
- a_mask: int32 [4, 8, 32], P('layer', 'row', 'col'), may hold values from 0 to 1, as said below
- b_dense: float32 [16384, 16384], P('row', ('col', 'layer')), may hold values from -0.21875 to 0.21875
- b_mask: int32 [128, 128], P('row', ('col', 'layer')), may hold values from 0 to 1, as said below
Outputs:
- product: float32 [1024, 16384], P('row', ('col', 'layer'))
The draws below stay inside these ranges and needn't reach their ends.
Inputs may be any that keep to these rules, and one draw needn't show every extreme that they name: For each l, each run of 4 block rows starting at a multiple of 4 and each run of 8 block columns starting at a multiple of 8, those blocks of a_mask[l] hold 1 to 12 ones. In every draw, for some l and some row run, the groups of all 4 column runs hold exactly 12. `b_mask`: take the block rows r * 64 to (r + 1) * 64 - 1, a residue d modulo 4, and the block columns g * 8 to (g + 1) * 8 - 1: the blocks among them whose row index is d modulo 4 hold 1 to 48 ones. In every draw, for some r, d and c, the groups of all g from c * 4 to c * 4 + 3 hold exactly 48.
All inputs are finite; a program needn't handle non-finite values.
Results may differ from the reference program's by a relative error of at most 0.00007.
Values sent between devices are 32-bit elements; how exact they have to be, the bound alone decides.
No kernel may reach another device: no remote copies, remote signals or barrier semaphores. Data moves between devices by JAX's collectives and lax.ppermute only.
A program may use at most 256 MiB of HBM per device.

```python
import jax
import jax.numpy as jnp
from jax import lax

BS = 128
K = 16384
N = 16384
MBR = 4
M = 1024
KB = 128
NB = 128
KBL = 32
KRB = 64
JCB = 8
QC = 8
XCAP = 48
ACAP = 12
N_ROW = 2
N_COL = 4
N_LAYER = 4


def draw_a_mask(key, part):
    members = MBR * QC
    groups = N_LAYER * N_ROW * N_COL
    count_key = jax.random.fold_in(key, 11)
    order_key = jax.random.fold_in(key, 12)
    layer_key = jax.random.fold_in(key, 13)
    row_key = jax.random.fold_in(key, 14)
    counts = jax.random.randint(count_key, (N_LAYER, N_ROW, N_COL), 1, ACAP + 1)
    layer_pick = jax.random.randint(layer_key, (), 0, N_LAYER)
    row_pick = jax.random.randint(row_key, (), 0, N_ROW)
    layer_ids = jnp.arange(N_LAYER)[:, None, None]
    row_ids = jnp.arange(N_ROW)[None, :, None]
    counts = jnp.where((layer_ids == layer_pick) & (row_ids == row_pick), ACAP, counts)

    def shuffle(group_key):
        return jax.random.permutation(group_key, members)
    orders = jax.vmap(shuffle)(jax.random.split(order_key, groups))
    occupied = (orders.reshape(N_LAYER, N_ROW, N_COL, members) < counts[..., None]).astype(jnp.int32)
    shaped = occupied.reshape(N_LAYER, N_ROW, N_COL, MBR, QC).transpose(0, 1, 3, 2, 4)
    return shaped.reshape(N_LAYER, N_ROW * MBR, N_COL * QC)


def draw_b_mask(key, part):
    per_layer = KRB // N_LAYER
    members = per_layer * JCB
    runs = N_COL * N_LAYER
    groups = N_ROW * N_LAYER * runs
    count_key = jax.random.fold_in(key, 21)
    order_key = jax.random.fold_in(key, 22)
    row_key = jax.random.fold_in(key, 23)
    residue_key = jax.random.fold_in(key, 24)
    col_key = jax.random.fold_in(key, 25)
    counts = jax.random.randint(count_key, (N_ROW, N_LAYER, runs), 1, XCAP + 1)
    row_pick = jax.random.randint(row_key, (), 0, N_ROW)
    residue_pick = jax.random.randint(residue_key, (), 0, N_LAYER)
    col_pick = jax.random.randint(col_key, (), 0, N_COL)
    row_ids = jnp.arange(N_ROW)[:, None, None]
    residue_ids = jnp.arange(N_LAYER)[None, :, None]
    run_ids = jnp.arange(runs)[None, None, :]
    forced = (row_ids == row_pick) & (residue_ids == residue_pick) & (run_ids // N_LAYER == col_pick)
    counts = jnp.where(forced, XCAP, counts)

    def shuffle(group_key):
        return jax.random.permutation(group_key, members)
    orders = jax.vmap(shuffle)(jax.random.split(order_key, groups))
    occupied = (orders.reshape(N_ROW, N_LAYER, runs, members) < counts[..., None]).astype(jnp.int32)
    shaped = occupied.reshape(N_ROW, N_LAYER, runs, per_layer, JCB).transpose(0, 3, 1, 2, 4)
    return shaped.reshape(KB, NB)


def steps_of(rng, dims, shards, least, top_value):
    factor_of = 1.0
    for dim, shards_of in shards:
        heights = jax.random.uniform(jax.random.fold_in(jax.random.fold_in(rng, 6), dim), (shards_of,), jnp.float32, least / len(shards), top_value / len(shards))
        factor_of = factor_of * jnp.repeat(jnp.exp(heights), dims[dim] // shards_of).reshape((-1,) + (1,) * (len(dims) - 1 - dim))
    return factor_of


def normal_values(stream_key, extent, deviation, bound, shards=(), dtype=jnp.bfloat16):
    factor_of = steps_of(stream_key, extent, shards, -0.22, 0.18) if shards else 1.0
    values = jax.random.normal(stream_key, extent, jnp.float32) * deviation * factor_of
    return jnp.minimum(jnp.maximum(values, -bound), bound).astype(dtype)


def setup_inputs(seed: int = 0) -> dict:
    seeds = jax.random.split(jax.random.key(seed), 5)
    return {
        "a_cyclic": normal_values(seeds[0], (N_LAYER, M, KBL * BS), 1.0, 6.0, ((0, 4), (1, 2), (2, 4)), jnp.float32),
        "a_mask": draw_a_mask(jax.random.fold_in(seeds[4], 71), 0),
        "b_dense": normal_values(seeds[2], (K, N), (K // 20) ** -0.5, 0.21875, ((0, 2), (1, 16)), jnp.float32),
        "b_mask": draw_b_mask(jax.random.fold_in(seeds[4], 71), 0),
    }


def reference(a_cyclic, a_mask, b_dense, b_mask):
    layers, row_count, columns = a_cyclic.shape
    q_count = columns // BS
    a_scale = jnp.repeat(jnp.repeat(a_mask.astype(jnp.float32), BS, axis=1), BS, axis=2)
    masked = a_cyclic * a_scale
    a_full = masked.reshape(layers, row_count, q_count, BS).transpose(1, 2, 0, 3).reshape(row_count, layers * columns)
    b_scale = jnp.repeat(jnp.repeat(b_mask.astype(jnp.float32), BS, axis=0), BS, axis=1)
    b_full = b_dense * b_scale
    return jnp.dot(a_full, b_full, preferred_element_type=jnp.float32, precision=lax.Precision.HIGHEST)
```

```python
import jax
import jax.numpy as jnp
from jax import lax
from jax.experimental import pallas as pl
from jax.experimental.pallas import tpu as pltpu
from jax.sharding import PartitionSpec as P

META = 8
GROUP = 4


def pack_unit(a_local, a_mask, cap, bs):
    row_blocks, q_blocks = a_mask.shape

    def body(mask_ref, a_ref, out_ref, meta_ref, sem, meta_sem):
        lane = lax.broadcasted_iota(jnp.int32, (META, bs), 1)
        meta_ref[...] = jnp.full((META, bs), -1.0, jnp.float32)

        def visit(g, n):
            i = g // q_blocks
            q = g % q_blocks
            live = mask_ref[i, q] > 0

            @pl.when(live)
            def _():
                pltpu.make_async_copy(
                    a_ref.at[pl.ds(i * bs, bs), pl.ds(q * bs, bs)],
                    out_ref.at[pl.ds(n * bs, bs), :],
                    sem,
                ).start()
                meta_ref[...] = jnp.where(lane == n, g.astype(jnp.float32), meta_ref[...])

            return n + live.astype(jnp.int32)

        count = lax.fori_loop(0, row_blocks * q_blocks, visit, jnp.int32(0))
        meta_copy = pltpu.make_async_copy(meta_ref, out_ref.at[pl.ds(cap * bs, META), :], meta_sem)
        meta_copy.start()

        def drain(n, carry):
            pltpu.make_async_copy(
                a_ref.at[pl.ds(0, bs), pl.ds(0, bs)], out_ref.at[pl.ds(0, bs), :], sem
            ).wait()
            return carry

        lax.fori_loop(0, count, drain, 0)
        meta_copy.wait()

    return pl.pallas_call(
        body,
        out_shape=jax.ShapeDtypeStruct((cap * bs + META, bs), jnp.float32),
        in_specs=[
            pl.BlockSpec(memory_space=pltpu.SMEM),
            pl.BlockSpec(memory_space=pl.ANY),
        ],
        out_specs=pl.BlockSpec(memory_space=pl.ANY),
        scratch_shapes=[
            pltpu.VMEM((META, bs), jnp.float32),
            pltpu.SemaphoreType.DMA,
            pltpu.SemaphoreType.DMA,
        ],
        name="pack_unit",
    )(a_mask, a_local)


def split_wide(x):
    hi = x.astype(jnp.bfloat16)
    lo = (x - hi.astype(jnp.float32)).astype(jnp.bfloat16)
    return jnp.concatenate([hi, lo], axis=1)


def multiply_run(codes, first_unit, units, b_mask, b_dense, row_blocks, cap, b_cap, bs):
    n_src = codes.shape[0]
    k_run, j_run = b_mask.shape
    pad = k_run + GROUP

    def body(code_ref, first_ref, bm_ref, u_ref, b_ref, out_ref,
             a_f32, a_wide, b_f32, acc, any_a, klist, blist, count, a_sem, b_sem, o_sem):
        first = first_ref[0]

        def load(u, carry):
            pltpu.make_async_copy(
                u_ref.at[first + u, pl.ds(0, cap * bs), :], a_f32.at[pl.ds(u * cap * bs, cap * bs), :], a_sem
            ).start()
            return carry

        lax.fori_loop(0, n_src, load, 0)

        def clear(k, carry):
            any_a[k] = 0
            return carry

        lax.fori_loop(0, k_run, clear, 0)

        def mark(t, carry):
            code = code_ref[t // cap, t % cap]

            @pl.when(code >= 0)
            def _():
                any_a[code // row_blocks] = 1

            return carry

        lax.fori_loop(0, n_src * cap, mark, 0)
        for j in range(j_run):
            count[j] = 0

        def plan(k, nb):
            used = any_a[k] > 0
            for j in range(j_run):
                live = jnp.logical_and(used, bm_ref[k, j] > 0)

                @pl.when(live)
                def _(j=j, nb=nb):
                    n = count[j]
                    klist[j, n] = k
                    blist[j, n] = nb
                    count[j] = n + 1
                    pltpu.make_async_copy(
                        b_ref.at[pl.ds(k * bs, bs), pl.ds(j * bs, bs)], b_f32.at[nb], b_sem
                    ).start()

                nb = nb + live.astype(jnp.int32)
            return nb

        total = lax.fori_loop(0, k_run, plan, jnp.int32(0))
        for j in range(j_run):
            n = count[j]
            for extra in range(GROUP):
                klist[j, n + extra] = 0
                blist[j, n + extra] = b_cap
        b_f32[b_cap] = jnp.zeros((bs, bs), jnp.float32)

        def wipe(k, carry):
            a_wide[k] = jnp.zeros((row_blocks * bs, 2 * bs), jnp.bfloat16)
            return carry

        lax.fori_loop(0, k_run, wipe, 0)

        def arrive(u, carry):
            pltpu.make_async_copy(
                u_ref.at[0, pl.ds(0, cap * bs), :], a_f32.at[pl.ds(0, cap * bs), :], a_sem
            ).wait()
            return carry

        lax.fori_loop(0, n_src, arrive, 0)

        def spread(t, carry):
            code = code_ref[t // cap, t % cap]

            @pl.when(code >= 0)
            def _():
                row = pl.multiple_of((code % row_blocks) * bs, bs)
                src = pl.multiple_of(t * bs, bs)
                a_wide[code // row_blocks, pl.ds(row, bs), :] = split_wide(a_f32[pl.ds(src, bs), :])

            return carry

        lax.fori_loop(0, n_src * cap, spread, 0)

        def b_arrive(n, carry):
            pltpu.make_async_copy(b_ref.at[pl.ds(0, bs), pl.ds(0, bs)], b_f32.at[0], b_sem).wait()
            return carry

        lax.fori_loop(0, total, b_arrive, 0)

        for j in range(j_run):
            acc[...] = jnp.zeros(acc.shape, jnp.float32)

            def step(t, carry, j=j):
                left = []
                right = []
                for e in range(GROUP):
                    n = t * GROUP + e
                    left.append(a_wide[klist[j, n]])
                    w = split_wide(b_f32[blist[j, n]])
                    right.extend([w, w])
                acc[...] += jnp.dot(
                    jnp.concatenate(left, axis=1),
                    jnp.concatenate(right, axis=0),
                    preferred_element_type=jnp.float32,
                )
                return carry

            lax.fori_loop(0, (count[j] + GROUP - 1) // GROUP, step, 0)
            out_ref[:, j * bs:(j + 1) * bs] = acc[:, :bs] + acc[:, bs:]

    return pl.pallas_call(
        body,
        out_shape=jax.ShapeDtypeStruct((row_blocks * bs, j_run * bs), jnp.float32),
        in_specs=[
            pl.BlockSpec(memory_space=pltpu.SMEM),
            pl.BlockSpec(memory_space=pltpu.SMEM),
            pl.BlockSpec(memory_space=pltpu.SMEM),
            pl.BlockSpec(memory_space=pl.ANY),
            pl.BlockSpec(memory_space=pl.ANY),
        ],
        out_specs=pl.BlockSpec(memory_space=pltpu.VMEM),
        scratch_shapes=[
            pltpu.VMEM((n_src * cap * bs, bs), jnp.float32),
            pltpu.VMEM((k_run, row_blocks * bs, 2 * bs), jnp.bfloat16),
            pltpu.VMEM((b_cap + 1, bs, bs), jnp.float32),
            pltpu.VMEM((row_blocks * bs, 2 * bs), jnp.float32),
            pltpu.SMEM((k_run,), jnp.int32),
            pltpu.SMEM((j_run, pad), jnp.int32),
            pltpu.SMEM((j_run, pad), jnp.int32),
            pltpu.SMEM((j_run,), jnp.int32),
            pltpu.SemaphoreType.DMA,
            pltpu.SemaphoreType.DMA,
            pltpu.SemaphoreType.DMA,
        ],
        name="multiply_run",
        compiler_params=pltpu.CompilerParams(vmem_limit_bytes=60 * 1024 * 1024),
    )(codes, first_unit, b_mask, units, b_dense)


def on_device(a_cyclic, a_mask, b_dense, b_mask):
    bs = a_cyclic.shape[1] // a_mask.shape[1]
    n_row, n_col, n_layer = lax.axis_size("row"), lax.axis_size("col"), lax.axis_size("layer")
    row_blocks, q_blocks = a_mask.shape[1:]
    k_run, j_run = b_mask.shape
    cap = max(2, row_blocks * q_blocks * 3 // 8)
    b_cap = n_layer * max(2, k_run // n_layer * j_run * 3 // 8)
    row = lax.axis_index("row")
    unit = pack_unit(a_cyclic[0], a_mask[0], cap, bs)
    layers = jnp.arange(n_layer, dtype=jnp.int32)

    if n_col % n_row == 0:
        wide = n_col // n_row
        pairs = []
        for r in range(n_row):
            for c in range(n_col):
                for l in range(n_layer):
                    src = (r * n_col + c) * n_layer + l
                    dst = ((c // wide) * n_col + r * wide + c % wide) * n_layer + l
                    pairs.append((src, dst))
        unit = lax.ppermute(unit, ("row", "col", "layer"), pairs)
        units = lax.all_gather(unit, ("col", "layer"), axis=0)
        per_run = wide * n_layer
        cols = jnp.arange(wide, dtype=jnp.int32)
    else:
        units = lax.all_gather(unit, ("row", "col", "layer"), axis=0)
        per_run = n_col * n_layer
        cols = jnp.arange(n_col, dtype=jnp.int32)
    ids = units[:, cap * bs, :cap].astype(jnp.int32).reshape(n_row, cols.shape[0], n_layer, cap)
    q = cols[None, :, None, None] * q_blocks + ids % q_blocks
    k = q * n_layer + layers[None, None, :, None]
    if n_col % n_row != 0:
        k = k - row * k_run
    live = (ids >= 0) & (k >= 0) & (k < k_run)
    codes = jnp.where(live, k * row_blocks + ids // q_blocks, -1).reshape(n_row, per_run, cap)

    def run(r):
        return multiply_run(
            lax.dynamic_index_in_dim(codes, r, 0, keepdims=False),
            jnp.reshape(r * per_run, (1,)).astype(jnp.int32),
            units, b_mask, b_dense, row_blocks, cap, b_cap, bs,
        )

    if n_row == 2:
        theirs = run(1 - row)
        received = lax.ppermute(theirs, "row", [(0, 1), (1, 0)])
        return run(row) + received
    partial = jnp.concatenate([run(jnp.int32(r)) for r in range(n_row)], axis=0)
    return lax.psum_scatter(partial, "row", scatter_dimension=0, tiled=True)


def solution(mesh):
    placed = (
        P("layer", "row", "col"),
        P("layer", "row", "col"),
        P("row", ("col", "layer")),
        P("row", ("col", "layer")),
    )
    return jax.shard_map(
        on_device, mesh=mesh, in_specs=placed, out_specs=P("row", ("col", "layer")), check_vma=False
    )
```

```python
import jax
import jax.numpy as jnp
from jax import lax
from jax.experimental import pallas as pl
from jax.experimental.pallas import tpu as pltpu
from jax.sharding import PartitionSpec as P

META = 8
GROUP = 4
CHUNK = 8
PARTS = 2
SPLIT = 4
AXES = ("row", "col", "layer")
SMEM = pl.BlockSpec(memory_space=pltpu.SMEM)
VMEM = pl.BlockSpec(memory_space=pltpu.VMEM)
ANY = pl.BlockSpec(memory_space=pl.ANY)
HBM = pl.BlockSpec(memory_space=pltpu.HBM)


def split_wide(x):
    hi = x.astype(jnp.bfloat16)
    lo = (x - hi.astype(jnp.float32)).astype(jnp.bfloat16)
    return jnp.concatenate([hi, lo], axis=1)


def pack_units(base, a_local, a_mask, slots, n_layer, bs):
    row_blocks, q_blocks = a_mask.shape
    rows = slots * bs + META

    def body(base_ref, mask_ref, a_ref, out_ref, sem):
        lane = lax.broadcasted_iota(jnp.int32, (META, bs), 1)

        def visit(i, carry):
            n, codes = carry
            for q in range(q_blocks):
                live = mask_ref[i, q] > 0
                code = ((base_ref[0] * q_blocks + q) * n_layer + base_ref[1]) * row_blocks + i

                @pl.when(live)
                def _(n=n, q=q):
                    part = jnp.int32(0)
                    for p in range(1, PARTS):
                        part = part + (n >= p * slots).astype(jnp.int32)
                    pltpu.make_async_copy(
                        a_ref.at[pl.ds(pl.multiple_of(i * bs, bs), bs), pl.ds(q * bs, bs)],
                        out_ref.at[part, pl.ds(pl.multiple_of((n - part * slots) * bs, bs), bs), :],
                        sem,
                    ).start()

                value = jnp.where(live, code, -1).astype(jnp.float32)
                codes = tuple(jnp.where(lane == n - p * slots, value, codes[p]) for p in range(PARTS))
                n = n + live.astype(jnp.int32)
            return n, codes

        empty = jnp.full((META, bs), -1.0, jnp.float32)
        count, codes = lax.fori_loop(0, row_blocks, visit, (jnp.int32(0), (empty,) * PARTS))
        for p in range(PARTS):
            out_ref[p, pl.ds(slots * bs, META), :] = codes[p]

        def drain(n, carry):
            pltpu.make_async_copy(
                a_ref.at[pl.ds(0, bs), pl.ds(0, bs)], out_ref.at[0, pl.ds(0, bs), :], sem
            ).wait()
            return carry

        lax.fori_loop(0, count, drain, 0)

    return pl.pallas_call(
        body,
        out_shape=jax.ShapeDtypeStruct((PARTS, rows, bs), jnp.float32),
        in_specs=[SMEM, SMEM, ANY],
        out_specs=VMEM,
        scratch_shapes=[pltpu.SemaphoreType.DMA],
        name="pack_units",
    )(base, a_mask, a_local)


def pack_b(b_mask, b_dense, b_cap, bs):
    k_run, j_run = b_mask.shape
    slots = (-(-b_cap // CHUNK) + j_run) * CHUNK

    def body(bm_ref, b_ref, out_ref, k_ref, start_ref, count_ref, b_f32, b_wide, sem, out_sem):
        def column(j, carry):
            n, live_blocks = carry
            start_ref[j] = n
            col = pl.multiple_of(j * bs, bs)

            def visit(t, n):
                for e in range(4):
                    k = t * 4 + e
                    live = bm_ref[k, j] > 0

                    @pl.when(live)
                    def _(k=k, n=n):
                        k_ref[n] = k
                        pltpu.make_async_copy(
                            b_ref.at[pl.ds(pl.multiple_of(k * bs, bs), bs), pl.ds(col, bs)], b_f32.at[n], sem
                        ).start()

                    n = n + live.astype(jnp.int32)
                return n

            m = lax.fori_loop(0, k_run // 4, visit, n)
            count_ref[j] = m
            return (m + CHUNK - 1) // CHUNK * CHUNK, live_blocks + m - n

        n, blocks = lax.fori_loop(0, j_run, column, (jnp.int32(0), jnp.int32(0)))
        start_ref[j_run] = n
        chunks = n // CHUNK
        b_wide[slots] = jnp.zeros((bs, 2 * bs), jnp.bfloat16)
        zero = pltpu.make_async_copy(b_wide.at[pl.ds(slots, 1)], out_ref.at[pl.ds(slots, 1)], out_sem.at[0])
        zero.start()

        def arrive(t, carry):
            pltpu.make_async_copy(b_ref.at[pl.ds(0, bs), pl.ds(0, bs)], b_f32.at[0], sem).wait()
            return carry

        lax.fori_loop(0, blocks, arrive, 0)

        def widen(t, carry):
            for e in range(CHUNK):
                b_wide[t * CHUNK + e] = split_wide(b_f32[t * CHUNK + e])
            pltpu.make_async_copy(
                b_wide.at[pl.ds(t * CHUNK, CHUNK)], out_ref.at[pl.ds(t * CHUNK, CHUNK)], out_sem.at[1]
            ).start()
            return carry

        lax.fori_loop(0, chunks, widen, 0)

        def leave(t, carry):
            pltpu.make_async_copy(
                b_wide.at[pl.ds(0, CHUNK)], out_ref.at[pl.ds(0, CHUNK)], out_sem.at[1]
            ).wait()
            return carry

        lax.fori_loop(0, chunks, leave, 0)
        zero.wait()

    return pl.pallas_call(
        body,
        out_shape=(
            jax.ShapeDtypeStruct((slots + 1, bs, 2 * bs), jnp.bfloat16),
            jax.ShapeDtypeStruct((slots,), jnp.int32),
            jax.ShapeDtypeStruct((j_run + 1,), jnp.int32),
            jax.ShapeDtypeStruct((j_run,), jnp.int32),
        ),
        in_specs=[SMEM, ANY],
        out_specs=(ANY, SMEM, SMEM, SMEM),
        scratch_shapes=[
            pltpu.VMEM((slots, bs, bs), jnp.float32),
            pltpu.VMEM((slots + 1, bs, 2 * bs), jnp.bfloat16),
            pltpu.SemaphoreType.DMA,
            pltpu.SemaphoreType.DMA((2,)),
        ],
        name="pack_b",
        compiler_params=pltpu.CompilerParams(vmem_limit_bytes=60 * 1024 * 1024),
    )(b_mask, b_dense)


def multiply_run(units, packed, k_run, row_blocks, slots, bs, columns=None, k_base=None):
    b_wide, b_k, b_start, b_end = packed
    b_slots = b_wide.shape[0] - 1
    j_from, j_to = columns or (0, b_end.shape[0])
    j_run = j_to - j_from
    arrays = list(dict.fromkeys(id(x) for x, _ in units))
    held = {id(x): x for x, _ in units}
    places = [(arrays.index(id(x)), at) for x, at in units]
    n_src = len(units)
    pad = k_run + GROUP
    split = SPLIT if row_blocks % SPLIT == 0 else 1
    part = row_blocks * bs // split
    per_part = row_blocks // split
    height = row_blocks * bs
    row_bits = row_blocks.bit_length() - 1 if row_blocks & (row_blocks - 1) == 0 else None

    def body(bk_ref, bs_ref, be_ref, base_ref, bw_ref, *rest):
        u_refs = [rest[ref].at[at] for ref, at in places]
        (out_ref, a_f32, a_wide, b_all, acc, codes, any_a, klist, blist,
         c_sem, a_sem, b_sem, z_sem) = rest[len(arrays):]
        for u in range(n_src):
            pltpu.make_async_copy(u_refs[u].at[pl.ds(slots * bs, META), :], codes.at[u], c_sem).start()
        for u in range(n_src):
            pltpu.make_async_copy(u_refs[u].at[pl.ds(0, slots * bs), :], a_f32.at[u], a_sem.at[u]).start()

        def b_copy(t, j):
            return pltpu.make_async_copy(
                bw_ref.at[pl.ds(t * CHUNK, CHUNK)], b_all.at[pl.ds(t * CHUNK, CHUNK)], b_sem.at[j]
            )

        for j in range(j_run):
            def b_load(t, carry, j=j):
                b_copy(t, j).start()
                return carry

            lax.fori_loop(bs_ref[j_from + j] // CHUNK, bs_ref[j_from + j + 1] // CHUNK, b_load, 0)
        zero = pltpu.make_async_copy(bw_ref.at[pl.ds(b_slots, 1)], b_all.at[pl.ds(b_slots, 1)], z_sem)
        zero.start()

        def wipe(k, carry):
            for r in range(split):
                any_a[k * split + r] = 0
            a_wide[k] = jnp.zeros((height, 2 * bs), jnp.bfloat16)
            return carry

        lax.fori_loop(0, k_run, wipe, 0)
        for u in range(n_src):
            pltpu.make_async_copy(u_refs[u].at[pl.ds(slots * bs, META), :], codes.at[u], c_sem).wait()
        base = base_ref[0] * (k_run * row_blocks)
        for u in range(n_src):
            pltpu.make_async_copy(
                u_refs[u].at[pl.ds(0, slots * bs), :], a_f32.at[u], a_sem.at[u]
            ).wait()

            for s in range(slots):
                code = codes[u, 0, s].astype(jnp.int32) - base
                live = jnp.logical_and(code >= 0, code < k_run * row_blocks)
                code = jnp.where(live, code, k_run * row_blocks)
                k = lax.shift_right_logical(code, row_bits) if row_bits is not None else code // row_blocks
                row = pl.multiple_of((code - k * row_blocks) * bs, bs)
                any_a[code // per_part] = 1
                a_wide[k, pl.ds(row, bs), :] = split_wide(a_f32[u, s * bs:(s + 1) * bs, :])

        zero.wait()

        for j in range(j_run):
            def choose(t, taken):
                k = bk_ref[t]
                out = []
                for r in range(split):
                    klist[r, taken[r]] = k
                    blist[r, taken[r]] = t
                    out.append(taken[r] + any_a[k * split + r])
                return tuple(out)

            taken = lax.fori_loop(
                bs_ref[j_from + j], be_ref[j_from + j], choose, (jnp.int32(0),) * split
            )
            longest = taken[0]
            for r in range(1, split):
                longest = jnp.maximum(longest, taken[r])
            groups = (longest + GROUP - 1) // GROUP
            for r in range(split):
                def blank(n, carry, r=r):
                    klist[r, n] = 0
                    blist[r, n] = b_slots
                    return carry

                lax.fori_loop(taken[r], groups * GROUP, blank, 0)

            def b_arrive(t, carry, j=j):
                b_copy(t, j).wait()
                return carry

            lax.fori_loop(bs_ref[j_from + j] // CHUNK, bs_ref[j_from + j + 1] // CHUNK, b_arrive, 0)
            acc[...] = jnp.zeros(acc.shape, jnp.float32)

            def step(t, carry):
                for r in range(split):
                    rows = slice(r * part, (r + 1) * part)
                    left = []
                    right = []
                    for e in range(GROUP):
                        left.append(a_wide[klist[r, t * GROUP + e], rows, :])
                        w = b_all[blist[r, t * GROUP + e]]
                        right.extend([w, w])
                    acc[rows, :] += jnp.dot(
                        jnp.concatenate(left, axis=1),
                        jnp.concatenate(right, axis=0),
                        preferred_element_type=jnp.float32,
                    )
                return carry

            lax.fori_loop(0, groups, step, 0)
            out_ref[:, j * bs:(j + 1) * bs] = acc[:, :bs] + acc[:, bs:]

    limit = (n_src * slots * bs * bs * 4 + (k_run + 1) * height * 4 * bs + (b_slots + 1) * bs * bs * 4
             + height * 2 * bs * 4 + height * j_run * bs * 4) * 17 // 16 + (2 << 20)
    if k_base is None:
        k_base = jnp.zeros((1,), jnp.int32)
    return pl.pallas_call(
        body,
        out_shape=jax.ShapeDtypeStruct((height, j_run * bs), jnp.float32),
        in_specs=[SMEM, SMEM, SMEM, SMEM, HBM] + [ANY] * len(arrays),
        out_specs=VMEM,
        scratch_shapes=[
            pltpu.VMEM((n_src, slots * bs, bs), jnp.float32),
            pltpu.VMEM((k_run + 1, height, 2 * bs), jnp.bfloat16),
            pltpu.VMEM((b_slots + 1, bs, 2 * bs), jnp.bfloat16),
            pltpu.VMEM((height, 2 * bs), jnp.float32),
            pltpu.SMEM((n_src, META, bs), jnp.float32),
            pltpu.SMEM(((k_run + 1) * split,), jnp.int32),
            pltpu.SMEM((split, pad), jnp.int32),
            pltpu.SMEM((split, pad), jnp.int32),
            pltpu.SemaphoreType.DMA,
            pltpu.SemaphoreType.DMA((n_src,)),
            pltpu.SemaphoreType.DMA((j_run,)),
            pltpu.SemaphoreType.DMA,
        ],
        name="multiply_run",
        compiler_params=pltpu.CompilerParams(vmem_limit_bytes=limit),
    )(b_k, b_start, b_end, k_base, b_wide, *[held[key] for key in arrays])


def on_device(a_cyclic, a_mask, b_dense, b_mask):
    bs = a_cyclic.shape[1] // a_mask.shape[1]
    n_row, n_col, n_layer = (lax.axis_size(name) for name in AXES)
    row_blocks, q_blocks = a_mask.shape[1:]
    k_run, j_run = b_mask.shape
    cap = max(2, row_blocks * q_blocks * 3 // 8)
    slots = -(-cap // PARTS)
    b_cap = n_layer * max(2, k_run // n_layer * j_run * 3 // 8)
    row, col, layer = (lax.axis_index(name) for name in AXES)
    paired = n_row == 2 and n_col % 2 == 0
    wide = n_col // 2 if paired else n_col
    base = jnp.stack([col % wide, layer]).astype(jnp.int32)
    packed_a = pack_units(base, a_cyclic[0], a_mask[0], slots, n_layer, bs)
    packed_b = pack_b(b_mask, b_dense, b_cap, bs)
    size = (k_run, row_blocks, slots, bs)

    if not paired:
        units = lax.all_gather(packed_a, AXES, axis=0)
        units = units.reshape((-1,) + packed_a.shape[1:])
        per_run = n_col * n_layer * PARTS
        k_base = jnp.reshape(row, (1,)).astype(jnp.int32)
        partial = jnp.concatenate(
            [
                multiply_run([(units, r * per_run + u) for u in range(per_run)], packed_b, *size, k_base=k_base)
                for r in range(n_row)
            ],
            axis=0,
        )
        return lax.psum_scatter(partial, "row", scatter_dimension=0, tiled=True)

    def send(x, target):
        pairs = []
        for r in range(n_row):
            for h in range(2):
                for w in range(wide):
                    for l in range(n_layer):
                        to = target(r, h, w, l)
                        if to is None:
                            continue
                        tr, th, tw, tl = to
                        pairs.append((
                            (r * n_col + h * wide + w) * n_layer + l,
                            (tr * n_col + th * wide + tw) * n_layer + tl,
                        ))
        return lax.ppermute(x, AXES, pairs)

    power = n_layer & (n_layer - 1) == 0

    def along(m):
        if power:
            return lambda r, h, w, l: (r, h, w, l ^ m)
        return lambda r, h, w, l: (r, h, w, (l + m) % n_layer)

    def collect(mine):
        if n_layer == 4:
            over2 = send(mine, along(2))
            line = [mine, send(mine, along(1)), over2, send(over2, along(1))]
        else:
            line = [mine] + [send(mine, along(m)) for m in range(1, n_layer)]
        plane = line + [send(x, lambda r, h, w, l: (r, 1 - h, w, l)) for x in line]
        twin = [send(x, lambda r, h, w, l: (r, h, (w + d) % wide, l)) for d in range(1, wide) for x in plane]
        return [(x, at) for x in plane + twin for at in range(x.shape[0])]

    home = (col // wide) == row
    far = send(packed_a[1:], lambda r, h, w, l: None if r == h else (h, 1 - h, w, l))
    near = send(packed_a[:1], lambda r, h, w, l: (h, 1 - h if r == h else h, w, l))
    near, far, packed_b = lax.optimization_barrier((near, far, packed_b))
    theirs = collect(jnp.where(home, near, far))
    ours = collect(jnp.where(home, packed_a[1:], near))
    cut = j_run * 3 // 8
    parts = []
    for columns in ((0, cut), (cut, j_run)):
        part = multiply_run(theirs, packed_b, *size, columns=columns)
        parts.append(send(part, lambda r, h, w, l: (1 - r, h, w, l)))
    ours = multiply_run(ours, packed_b, *size)
    return ours + jnp.concatenate(parts, axis=1)


def solution(mesh):
    placed = (
        P("layer", "row", "col"),
        P("layer", "row", "col"),
        P("row", ("col", "layer")),
        P("row", ("col", "layer")),
    )
    return jax.shard_map(
        on_device, mesh=mesh, in_specs=placed, out_specs=P("row", ("col", "layer")), check_vma=False
    )
```
